32 devices in a mesh: gx: 4 (over x, core), gy: 4 (over z), gz: 2 (over y).
Axes of the slice: x: 2, y: 2, z: 4, core: 2. Of those that a mesh axis runs over, the one named last changes fastest.
Arguments:
- field: bfloat16 [1, 64, 16, 32, 256], P(None, None, 'gx', 'gy', 'gz'), may hold values from -6 to 6
- kernel_one: bfloat16 [3, 3, 3, 64, 64], replicated, may hold values from -0.15625 to 0.15625
- bias_one: float32 [64], replicated, may hold values from -3 to 3
- kernel_two: bfloat16 [3, 3, 3, 64, 64], replicated, may hold values from -0.15625 to 0.15625
- bias_two: float32 [64], replicated, may hold values from -3 to 3
- kernel_three: bfloat16 [3, 3, 3, 64, 64], replicated, may hold values from -0.15625 to 0.15625
- bias_three: float32 [64], replicated, may hold values from -3 to 3
Outputs:
- latent: bfloat16 [1, 64, 16, 32, 256], P(None, None, 'gx', 'gy', 'gz')
The draws below stay inside these ranges and needn't reach their ends.
All inputs are finite; a program needn't handle non-finite values.
Results may differ from the reference program's by a relative error of at most 0.0048.
Values may be sent and summed in bfloat16 or wider, within the bound.
No kernel may reach another device: no remote copies, remote signals or barrier semaphores. Data moves between devices by JAX's collectives and lax.ppermute only.
A program may use at most 256 MiB of HBM per device.

```python
import jax
import jax.numpy as jnp

C = 64
B = 1
NX = 16
NY = 32
NZ = 256


def shard_levels(key, dims, cuts, low, top_value):
    factor_of = 1.0
    for dim, blocks in cuts:
        steps = jax.random.uniform(jax.random.fold_in(jax.random.fold_in(key, 6), dim), (blocks,), jnp.float32, low / len(cuts), top_value / len(cuts))
        factor_of = factor_of * jnp.repeat(jnp.exp(steps), dims[dim] // blocks).reshape((-1,) + (1,) * (len(dims) - 1 - dim))
    return factor_of


def gaussian(stream_key, shape, deviation, reach, shards=(), dtype=jnp.bfloat16):
    entries = jax.random.normal(stream_key, shape, jnp.float32) * deviation
    if len(shards) > 0:
        entries = shard_levels(stream_key, shape, shards, -0.22, 0.18) * entries
    return jnp.clip(entries, min=-reach, max=reach).astype(dtype)


def setup_inputs(seed: int = 0) -> dict:
    arg_keys = jax.random.split(jax.random.key(seed), 8)
    return {
        "field": gaussian(arg_keys[0], (B, C, NX, NY, NZ), 1.0, 6.0, ((2, 4), (3, 4), (4, 2))),
        "kernel_one": gaussian(arg_keys[1], (3, 3, 3, C, C), (27 * C) ** -0.5, 0.15625),
        "bias_one": gaussian(arg_keys[2], (C,), 0.5, 3.0, (), jnp.float32),
        "kernel_two": gaussian(arg_keys[3], (3, 3, 3, C, C), (27 * C) ** -0.5, 0.15625),
        "bias_two": gaussian(arg_keys[4], (C,), 0.5, 3.0, (), jnp.float32),
        "kernel_three": gaussian(arg_keys[5], (3, 3, 3, C, C), (27 * C) ** -0.5, 0.15625),
        "bias_three": gaussian(arg_keys[6], (C,), 0.5, 3.0, (), jnp.float32),
    }


def layer(values, kernel, bias):
    total = jnp.zeros(values.shape, jnp.float32)
    for along_x in range(3):
        for along_y in range(3):
            for along_z in range(3):
                shifted = jnp.roll(values, (1 - along_x, 1 - along_y, 1 - along_z), axis=(2, 3, 4))
                matrix = kernel[along_x, along_y, along_z].astype(jnp.float32)
                total = total + jnp.einsum("oc,bcxyz->boxyz", matrix, shifted)
    total = total + bias.astype(jnp.float32)[None, :, None, None, None]
    return jax.nn.gelu(total, approximate=False).astype(jnp.bfloat16)


def reference(field, kernel_one, bias_one, kernel_two, bias_two, kernel_three, bias_three):
    first = layer(field.astype(jnp.float32), kernel_one, bias_one)
    second = layer(first.astype(jnp.float32), kernel_two, bias_two)
    return layer(second.astype(jnp.float32), kernel_three, bias_three)
```

```python
import jax
import jax.numpy as jnp
from jax import lax
from jax.experimental import pallas as pl
from jax.experimental.pallas import tpu as pltpu
from jax.sharding import PartitionSpec as P

HALO = 3
SQRT_HALF = 0.7071067811865476


def around(size):
    return -(-size // 16) * 16


def gelu(u):
    return 0.5 * u * (1.0 + lax.erf(u * SQRT_HALF))


def conv_line_block(source, x, first, lines, weight, bias):
    rows = source.shape[2]
    pieces = [
        source[x + a, first + e : first + e + lines].reshape(lines * rows, 128)
        for a in range(3)
        for e in range(3)
    ]
    stacked = jnp.concatenate(pieces, axis=1)
    both = lax.dot_general(
        stacked, weight, (((1,), (1,)), ((), ())), preferred_element_type=jnp.float32
    )
    here = both[:, :128]
    following = pltpu.roll(both[:, 128:], lines * rows - 1, 0)
    return gelu(here + following + bias).reshape(lines, rows, 128)


def layers_kernel(own, xm, xp, ym, yp, cm, cp, w1, w2, w3, b1, b2, b3, out, s0, s1, s2):
    nx, ny, rows, _ = own.shape
    h = HALO
    s0[h : h + nx, h : h + ny, :rows] = own[...]
    s0[:h, h : h + ny, :rows] = xm[...]
    s0[h + nx :, h : h + ny, :rows] = xp[...]
    s0[h : h + nx, :h, :rows] = ym[...]
    s0[h : h + nx, h + ny :, :rows] = yp[...]
    s0[:h, :h, :rows] = cm[:, :h]
    s0[:h, h + ny :, :rows] = cm[:, h:]
    s0[h + nx :, :h, :rows] = cp[:, :h]
    s0[h + nx :, h + ny :, :rows] = cp[:, h:]

    def layer(source, target, weight, bias, last):
        lines = source.shape[1] - 2

        def plane(x, carry):
            y = conv_line_block(source, x, 0, lines, weight[...], bias[...])
            y = y.astype(jnp.bfloat16)
            if last:
                target[x] = y[:, : target.shape[2]]
            else:
                target[x] = y
            return carry

        lax.fori_loop(0, source.shape[0] - 2, plane, 0)

    layer(s0, s1, w1, b1, False)
    layer(s1, s2, w2, b2, False)
    layer(s2, out, w3, b3, True)


def layers(own, xm, xp, ym, yp, cm, cp, ws, bs, pairs):
    nx, ny, rows, _ = own.shape
    pad = around(rows)
    h = HALO
    vm = pl.BlockSpec(memory_space=pltpu.VMEM)
    return pl.pallas_call(
        layers_kernel,
        out_shape=jax.ShapeDtypeStruct((nx, ny, pairs, 128), jnp.bfloat16),
        in_specs=[vm] * 13,
        out_specs=vm,
        scratch_shapes=[
            pltpu.VMEM((nx + 2 * k, ny + 2 * k, pad, 128), jnp.bfloat16)
            for k in (h, h - 1, h - 2)
        ],
        compiler_params=pltpu.CompilerParams(vmem_limit_bytes=60 * 1024 * 1024),
    )(own, xm, xp, ym, yp, cm, cp, *ws, *bs)


def folded(kernel):
    zero = jnp.zeros_like(kernel[:, :, 0])
    blocks = []
    for t in range(2):
        for q in range(2):
            taps = [p - q + 2 * t for p in range(2)]
            blocks.append(
                jnp.stack(
                    [kernel[:, :, f] if 0 <= f < 3 else zero for f in taps], axis=2
                )
            )
    w = jnp.stack(blocks, axis=0)
    _, _, _, _, o, c = w.shape
    return jnp.transpose(w, (0, 4, 1, 2, 3, 5)).reshape(4 * o, 18 * c)


def shift(x, axis, up):
    count = lax.axis_size(axis)
    pairs = [(i, (i + 1) % count) if up else ((i + 1) % count, i) for i in range(count)]
    return lax.ppermute(x, axis, pairs)


def swap_edges(tail, head, axis, dim):
    if lax.axis_size(axis) == 2:
        both = shift(jnp.concatenate([tail, head], axis=dim), axis, True)
        return jnp.split(both, 2, axis=dim)
    return shift(tail, axis, True), shift(head, axis, False)


def shards(field, kernel_one, bias_one, kernel_two, bias_two, kernel_three, bias_three):
    h = HALO
    ws = [folded(k) for k in (kernel_one, kernel_two, kernel_three)]
    bs = [jnp.concatenate([b, b])[None, :] for b in (bias_one, bias_two, bias_three)]
    _, c, nx, ny, nz = field.shape
    cells = jnp.transpose(field[0], (1, 2, 3, 0))
    left, right = swap_edges(cells[:, :, nz - h :], cells[:, :, :h], "gz", 2)
    own = jnp.concatenate([left, cells, right], axis=2)
    count = (nz + 2 * h) // 2
    rows = -(-count // 8) * 8
    own = own.reshape(nx, ny, count, 2 * c)
    own = jnp.pad(own, ((0, 0), (0, 0), (0, rows - count), (0, 0)))
    ym, yp = swap_edges(own[:, ny - h :], own[:, :h], "gy", 1)
    xm, xp = swap_edges(own[nx - h :], own[:h], "gx", 0)
    sides = jnp.concatenate([ym, yp], axis=1)
    cm, cp = swap_edges(sides[nx - h :], sides[:h], "gx", 0)
    out = layers(own, xm, xp, ym, yp, cm, cp, ws, bs, nz // 2)
    out = out.reshape(nx, ny, nz, c)
    return jnp.transpose(out, (3, 0, 1, 2))[None]


def solution(mesh):
    return jax.shard_map(
        shards,
        mesh=mesh,
        in_specs=(P(None, None, "gx", "gy", "gz"), P(), P(), P(), P(), P(), P()),
        out_specs=P(None, None, "gx", "gy", "gz"),
        check_vma=False,
    )
```

```python
import functools

import jax
import jax.numpy as jnp
from jax import lax
from jax.experimental import pallas as pl
from jax.experimental.pallas import tpu as pltpu
from jax.sharding import PartitionSpec as P

HALO = 3
SQRT_HALF = 0.7071067811865476
BF16 = jnp.bfloat16
F32 = jnp.float32
VMEM = pl.BlockSpec(memory_space=pltpu.VMEM)


def around(size, step):
    return -(-size // step) * step


def call(kernel, outs, scratch=(), name=None, flops=0, nbytes=0):
    outs = [jax.ShapeDtypeStruct(s, d) for s, d in outs]

    def run(*args):
        return pl.pallas_call(
            kernel,
            out_shape=outs,
            in_specs=[VMEM] * len(args),
            out_specs=[VMEM] * len(outs),
            scratch_shapes=list(scratch),
            name=name,
            cost_estimate=pl.CostEstimate(
                flops=flops, bytes_accessed=nbytes, transcendentals=0
            ),
            compiler_params=pltpu.CompilerParams(vmem_limit_bytes=48 * 1024 * 1024),
        )(*args)

    return run


def gelu(u):
    return 0.5 * u * (1.0 + lax.erf(u * SQRT_HALF))


def iota(shape, dim):
    return lax.broadcasted_iota(jnp.int32, shape, dim)


def rows_kernel(field, pairs, edges, planes):
    c, nx, ny, nz = field.shape
    rows = pairs.shape[2]
    m = iota((rows + 8, 2 * nz), 0)
    j = iota((rows + 8, 2 * nz), 1)
    half = nz // 2
    first = jnp.where(m < rows + 2, m - rows + half, m - rows - 1)
    m = jnp.where(m < rows, m, jnp.where(m < rows + 4, first, -8))
    second = (j >= nz).astype(jnp.int32)
    pick = (j - nz * second == 2 * m - 3 + second).astype(F32).astype(BF16)
    blank = jnp.zeros((c, nz), BF16)
    for x in range(nx):
        planes[x] = field[:, x].astype(F32).reshape(c * ny, nz)
        for y in range(0, ny, 2):
            blocks = []
            for k in range(2):
                b = planes[x, pl.ds(y + k, c, stride=ny), :].astype(BF16)
                blocks.append(jnp.concatenate([b, blank], axis=1))
                blocks.append(jnp.concatenate([blank, b], axis=1))
            r = lax.dot_general(
                pick,
                jnp.concatenate(blocks, axis=0),
                (((1,), (1,)), ((), ())),
                preferred_element_type=F32,
            ).astype(BF16)
            for k in range(2):
                lanes = slice(2 * c * k, 2 * c * (k + 1))
                pairs[x, y + k] = r[:rows, lanes]
                edges[x, y + k] = r[rows : rows + 4, lanes]


def faces_kernel(pairs, edges, own, xu, xd, yu, yd, wide):
    nx, ny, rows, _ = pairs.shape
    h = HALO
    wide[:, :, :4] = edges[...].astype(F32)
    got = wide[...]
    row = iota(got.shape, 2)
    low = jnp.where(row < 2, got, 0.0)
    moved = pltpu.roll(got, got.shape[2] - 1, 2)
    high = jnp.where((row >= 1) & (row < 3), moved, 0.0)
    e = pairs[...].astype(F32)
    e = jnp.concatenate(
        [e[:, :, :8] + low, e[:, :, 8 : rows - 8], e[:, :, rows - 8 :] + high], axis=2
    ).astype(BF16)
    own[...] = e
    xu[...] = e[nx - h :]
    xd[...] = e[:h]
    yu[...] = e[:, ny - h :]
    yd[...] = e[:, :h]


def weights_kernel(k1, k2, k3, b1, b2, b3, w1, w2, w3, bias):
    _, _, taps, o, c = k1.shape
    j = iota((taps * o, 8 * o), 0)
    n = iota((taps * o, 8 * o), 1)
    p = n // (4 * o)
    t = n // (2 * o) % 2
    q = n // o % 2
    pick = (j == (p - q + 2 * t) * o + n % o).astype(F32).astype(BF16)
    for k, w in ((k1, w1), (k2, w2), (k3, w3)):
        for a in range(3):
            for e in range(3):
                r = lax.dot_general(
                    k[a, e].reshape(taps * o, c),
                    pick,
                    (((0,), (0,)), ((), ())),
                    preferred_element_type=F32,
                ).astype(BF16)
                at = (a * 3 + e) * 2 * c
                w[at : at + c] = r[:, : 4 * o]
                w[at + c : at + 2 * c] = r[:, 4 * o :]
    for i, b in enumerate((b1, b2, b3)):
        bias[i : i + 1] = jnp.concatenate([b[...], b[...]], axis=1)


def conv(source, planes, starts, lines, weight, bias):
    rows = source.shape[2]
    height = lines * rows
    columns = []
    for a in range(3):
        for e in range(3):
            columns.append(
                jnp.concatenate(
                    [
                        source[x + a, s + e : s + e + lines].reshape(height, 128)
                        for x in planes
                        for s in starts
                    ],
                    axis=0,
                )
            )
    both = jnp.dot(
        jnp.concatenate(columns, axis=1), weight, preferred_element_type=F32
    )
    total = both.shape[0]
    u = both[:, :128] + pltpu.roll(both[:, 128:], total - 1, 0) + bias
    y = gelu(u).astype(BF16)
    return y.reshape(len(planes), len(starts) * lines, rows, 128)


def groups(count, size):
    return [list(range(i, min(i + size, count))) for i in range(0, count, size)]


def middle_kernel(own, xm, xp, w1, w2, w3, bias, l1, l2, l3, s0, s1):
    nx, ny, rows, _ = own.shape
    h = HALO
    s0[:h, :, :rows] = xm[...]
    s0[h : h + nx, :, :rows] = own[...]
    s0[h + nx :, :, :rows] = xp[...]
    for g in groups(nx + 4, 2):
        y = conv(s0, g, [0], ny - 2, w1[...], bias[0:1])
        for i, x in enumerate(g):
            s1[x] = y[i]
            l1[x, :2] = y[i, :2]
            l1[x, 2:] = y[i, ny - 4 :]
    for g in groups(nx + 2, 3):
        y = conv(s1, g, [0], ny - 4, w2[...], bias[1:2])
        for i, x in enumerate(g):
            l2[x] = y[i]
    for g in groups(nx, 4):
        y = conv(l2, g, [0], ny - 6, w3[...], bias[2:3])
        for i, x in enumerate(g):
            l3[x] = y[i, :, : l3.shape[2]]


def outer_kernel(
    own, xm, xp, ym, yp, cmm, cpm, cmp, cpp, l1, l2, l3, w1, w2, w3, bias,
    out, s0, s1, s2, stage,
):
    nx, ny, rows, _ = own.shape
    h = HALO
    for planes, below, core, above in (
        (slice(0, h), cmm, xm, cmp),
        (slice(h, h + nx), ym, own, yp),
        (slice(h + nx, h + nx + h), cpm, xp, cpp),
    ):
        s0[planes, :3, :rows] = below[...]
        s0[planes, 3:5, :rows] = core[:, :2]
        s0[planes, 5:7, :rows] = core[:, ny - 2 :]
        s0[planes, 7:, :rows] = above[...]
    s1[:, 3:7] = l1[...]
    inner = l2.shape[1]
    s2[:, 3:5] = l2[:, :2]
    s2[:, 5:7] = l2[:, inner - 2 :]
    for source, target, w, i in ((s0, s1, w1, 0), (s1, s2, w2, 1)):
        for g in groups(source.shape[0] - 2, 2):
            y = conv(source, g, [0, 5], 3, w[...], bias[i : i + 1])
            for k, x in enumerate(g):
                target[x, :3] = y[k, :3]
                target[x, 7:] = y[k, 3:]
    half = l3.shape[2]
    c = out.shape[0]
    nz = out.shape[3]
    deep, wide = 4 * half, 8 * nz
    r = iota((deep, wide), 0)
    n = iota((deep, wide), 1)
    side = n // (4 * nz)
    spread = (r // half == n // nz % 4) & (n % nz == 2 * (r % half) + side)
    spread = spread.astype(F32).astype(BF16)
    for g in groups(nx, 2):
        y = conv(s2, g, [0, 5], 3, w3[...], bias[2:3])
        for k, x in enumerate(g):
            lines = [y[k, i, :half] for i in range(3)]
            lines += [l3[x, i] for i in range(ny - 6)]
            lines += [y[k, i, :half] for i in range(3, 6)]
            for first in range(0, ny, 4):
                r = lax.dot_general(
                    jnp.concatenate(lines[first : first + 4], axis=0),
                    spread,
                    (((0,), (0,)), ((), ())),
                    preferred_element_type=F32,
                )
                r = r[:c, : 4 * nz] + r[c:, 4 * nz :]
                for i in range(4):
                    stage[x, pl.ds(first + i, c, stride=ny), :] = r[
                        :, i * nz : (i + 1) * nz
                    ]
            out[:, x] = stage[x].reshape(c, ny, nz).astype(BF16)


def shift(x, axis, up):
    count = lax.axis_size(axis)
    pairs = [(i, (i + 1) % count) if up else ((i + 1) % count, i) for i in range(count)]
    return lax.ppermute(x, axis, pairs)


def shards(field, kernel_one, bias_one, kernel_two, bias_two, kernel_three, bias_three):
    h = HALO
    field = field[0]
    c, nx, ny, nz = field.shape
    rows = around((nz + 2 * h) // 2, 8)
    pad = around(rows, 16)
    half = nz // 2
    line = 2 * c

    pairs, edges = call(
        rows_kernel,
        [((nx, ny, rows, line), BF16), ((nx, ny, 4, line), BF16)],
        [pltpu.VMEM((nx, c * ny, nz), F32)],
        name="rows",
    )(field)
    if lax.axis_size("gz") == 2:
        edges = shift(edges, "gz", True)
    else:
        edges = jnp.concatenate(
            [shift(edges[:, :, :2], "gz", True), shift(edges[:, :, 2:], "gz", False)],
            axis=2,
        )
    xface = ((h, ny, rows, line), BF16)
    yface = ((nx, h, rows, line), BF16)
    own, xu, xd, yu, yd = call(
        faces_kernel,
        [((nx, ny, rows, line), BF16), xface, xface, yface, yface],
        [pltpu.VMEM((nx, ny, 8, line), F32)],
        name="faces",
    )(pairs, edges)
    xm, xp = shift(xu, "gx", True), shift(xd, "gx", False)
    ym, yp = shift(yu, "gy", True), shift(yd, "gy", False)
    cmm, cpm = shift(ym[nx - h :], "gx", True), shift(ym[:h], "gx", False)
    cmp, cpp = shift(yp[nx - h :], "gx", True), shift(yp[:h], "gx", False)
    w1, w2, w3, bias = call(
        weights_kernel,
        [((18 * c, 4 * c), BF16)] * 3 + [((3, line), F32)],
        name="weights",
        flops=2 * 10**9,
        nbytes=10**6,
    )(
        kernel_one, kernel_two, kernel_three,
        bias_one[None], bias_two[None], bias_three[None],
    )
    ws = (w1, w2, w3, bias)
    l1, l2, l3 = call(
        middle_kernel,
        [
            ((nx + 4, 4, pad, line), BF16),
            ((nx + 2, ny - 4, pad, line), BF16),
            ((nx, ny - 6, half, line), BF16),
        ],
        [
            pltpu.VMEM((nx + 6, ny, pad, line), BF16),
            pltpu.VMEM((nx + 4, ny - 2, pad, line), BF16),
        ],
        name="middle",
        flops=6 * 10**9,
        nbytes=10**6,
    )(own, xm, xp, *ws)
    (out,) = call(
        outer_kernel,
        [((c, nx, ny, nz), BF16)],
        [
            pltpu.VMEM((nx + 6, 10, pad, line), BF16),
            pltpu.VMEM((nx + 4, 10, pad, line), BF16),
            pltpu.VMEM((nx + 2, 10, pad, line), BF16),
            pltpu.VMEM((nx, c * ny, nz), F32),
        ],
        name="outer",
        flops=8 * 10**9,
        nbytes=10**6,
    )(own, xm, xp, ym, yp, cmm, cpm, cmp, cpp, l1, l2, l3, *ws)
    return out[None]


def solution(mesh):
    return jax.shard_map(
        shards,
        mesh=mesh,
        in_specs=(P(None, None, "gx", "gy", "gz"), P(), P(), P(), P(), P(), P()),
        out_specs=P(None, None, "gx", "gy", "gz"),
        check_vma=False,
    )
```

```python
import jax
import jax.numpy as jnp
from jax import lax
from jax.experimental import pallas as pl
from jax.experimental.pallas import tpu as pltpu
from jax.sharding import PartitionSpec as P


HALO = 3
SQRT_HALF = 0.7071067811865476
BF16 = jnp.bfloat16
F32 = jnp.float32
VMEM = pl.BlockSpec(memory_space=pltpu.VMEM)


def around(size, step):
    return -(-size // step) * step


def call(kernel, outs, scratch=(), flops=0, nbytes=0):
    outs = [jax.ShapeDtypeStruct(s, d) for s, d in outs]

    def run(*args):
        return pl.pallas_call(
            kernel,
            out_shape=outs,
            in_specs=[VMEM] * len(args),
            out_specs=[VMEM] * len(outs),
            scratch_shapes=list(scratch),
            cost_estimate=pl.CostEstimate(
                flops=flops, bytes_accessed=nbytes, transcendentals=0
            ),
            compiler_params=pltpu.CompilerParams(vmem_limit_bytes=48 * 1024 * 1024),
        )(*args)

    return run


def gelu(u):
    return 0.5 * u * (1.0 + lax.erf(u * SQRT_HALF))


def iota(shape, dim):
    return lax.broadcasted_iota(jnp.int32, shape, dim)


def rows_kernel(field, pairs, edges, planes):
    c, nx, ny, nz = field.shape
    rows = pairs.shape[2]
    m = iota((rows + 8, 2 * nz), 0)
    j = iota((rows + 8, 2 * nz), 1)
    half = nz // 2
    first = jnp.where(m < rows + 2, m - rows + half, m - rows - 1)
    m = jnp.where(m < rows, m, jnp.where(m < rows + 4, first, -8))
    second = (j >= nz).astype(jnp.int32)
    pick = (j - nz * second == 2 * m - 3 + second).astype(F32).astype(BF16)
    blank = jnp.zeros((c, nz), BF16)
    for x in range(nx):
        planes[x] = field[:, x].astype(F32).reshape(c * ny, nz)
        for y in range(0, ny, 2):
            blocks = []
            for k in range(2):
                b = planes[x, pl.ds(y + k, c, stride=ny), :].astype(BF16)
                blocks.append(jnp.concatenate([b, blank], axis=1))
                blocks.append(jnp.concatenate([blank, b], axis=1))
            r = lax.dot_general(
                pick,
                jnp.concatenate(blocks, axis=0),
                (((1,), (1,)), ((), ())),
                preferred_element_type=F32,
            ).astype(BF16)
            for k in range(2):
                lanes = slice(2 * c * k, 2 * c * (k + 1))
                pairs[x, y + k] = r[:rows, lanes]
                edges[x, y + k] = r[rows : rows + 4, lanes]


def faces_kernel(pairs, edges, own, xu, xd, yu, yd, wide):
    nx, ny, rows, _ = pairs.shape
    h = HALO
    wide[:, :, :4] = edges[...].astype(F32)
    got = wide[...]
    row = iota(got.shape, 2)
    low = jnp.where(row < 2, got, 0.0)
    moved = pltpu.roll(got, got.shape[2] - 1, 2)
    high = jnp.where((row >= 1) & (row < 3), moved, 0.0)
    e = pairs[...].astype(F32)
    e = jnp.concatenate(
        [e[:, :, :8] + low, e[:, :, 8 : rows - 8], e[:, :, rows - 8 :] + high], axis=2
    ).astype(BF16)
    own[...] = e
    xu[...] = e[nx - h :]
    xd[...] = e[:h]
    yu[...] = e[:, ny - h :]
    yd[...] = e[:, :h]


def weights_kernel(k1, k2, k3, b1, b2, b3, w1, w2, w3, bias):
    _, _, taps, o, c = k1.shape
    j = iota((taps * o, 8 * o), 0)
    n = iota((taps * o, 8 * o), 1)
    p = n // (4 * o)
    t = n // (2 * o) % 2
    q = n // o % 2
    pick = (j == (p - q + 2 * t) * o + n % o).astype(F32).astype(BF16)
    for k, w in ((k1, w1), (k2, w2), (k3, w3)):
        for a in range(3):
            for e in range(3):
                r = lax.dot_general(
                    k[a, e].reshape(taps * o, c),
                    pick,
                    (((0,), (0,)), ((), ())),
                    preferred_element_type=F32,
                ).astype(BF16)
                at = (a * 3 + e) * 2 * c
                w[at : at + c] = r[:, : 4 * o]
                w[at + c : at + 2 * c] = r[:, 4 * o :]
    for i, b in enumerate((b1, b2, b3)):
        bias[i : i + 1] = jnp.concatenate([b[...], b[...]], axis=1)


def conv(source, x, lines, weight, bias):
    rows = source.shape[2]
    height = lines * rows
    taps = [
        source[x + a, e : e + lines].reshape(height, 128)
        for a in range(3)
        for e in range(3)
    ]
    both = jnp.dot(jnp.concatenate(taps, axis=1), weight, preferred_element_type=F32)
    u = both[:, :128] + pltpu.roll(both[:, 128:], height - 1, 0) + bias
    return gelu(u).astype(BF16).reshape(lines, rows, 128)


def strip_kernel(own, xm, xp, l1, w1, bias, s0):
    nx, ny, rows, _ = own.shape
    h = HALO
    s0[:h, :, :rows] = xm[...]
    s0[h : h + nx, :, :rows] = own[...]
    s0[h + nx :, :, :rows] = xp[...]
    for x in range(nx + 4):
        l1[x] = conv(s0, x, ny - 2, w1[...], bias[0:1])


def middle_first(own, xm, xp, w1, bias, l1, s0):
    strip_kernel(own, xm, xp, l1, w1, bias, s0)


def middle_second(l1, w2, w3, bias, l2, l3):
    lines = l1.shape[1]
    for x in range(l2.shape[0]):
        l2[x] = conv(l1, x, lines - 2, w2[...], bias[1:2])
    for x in range(l3.shape[0]):
        l3[x] = conv(l2, x, lines - 4, w3[...], bias[2:3])[:, : l3.shape[2]]


def spread_pattern(half, nz):
    r = iota((4 * half, 8 * nz), 0)
    n = iota((4 * half, 8 * nz), 1)
    hit = (r // half == n // nz % 4) & (n % nz == 2 * (r % half) + n // (4 * nz))
    return hit.astype(F32).astype(BF16)


def edge_strip(below, own, xm, xp, ym, cm, cp, l1, l2, ws, bias, s0, s1, s2):
    nx, ny, rows, _ = own.shape
    h = HALO
    inner = slice(0, 2) if below else slice(ny - 2, ny)
    near = slice(3, 5) if below else slice(0, 2)
    far = slice(0, 3) if below else slice(2, 5)
    for planes, core, side in (
        (slice(0, h), xm, cm),
        (slice(h, h + nx), own, ym),
        (slice(h + nx, h + nx + h), xp, cp),
    ):
        s0[planes, near, :rows] = core[:, inner]
        s0[planes, far, :rows] = side[...]
    n1, n2 = l1.shape[1], l2.shape[1]
    s1[:, near] = l1[:, :2] if below else l1[:, n1 - 2 :]
    s2[:, near] = l2[:, :2] if below else l2[:, n2 - 2 :]
    for source, target, i in ((s0, s1, 0), (s1, s2, 1)):
        for x in range(source.shape[0] - 2):
            target[x, far] = conv(source, x, 3, ws[i][...], bias[i : i + 1])
    return [conv(s2, x, 3, ws[2][...], bias[2:3]) for x in range(nx)]


def lower_kernel(own, xm, xp, ym, cm, cp, l1, l2, w1, w2, w3, bias, low, s0, s1, s2):
    y = edge_strip(
        True, own, xm, xp, ym, cm, cp, l1, l2, (w1, w2, w3), bias, s0, s1, s2
    )
    for x, lines in enumerate(y):
        low[x] = lines[:, : low.shape[2]]


def upper_kernel(
    own, xm, xp, yp, cm, cp, l1, l2, low, mid, w1, w2, w3, bias, out, s0, s1, s2, stage
):
    c, nx, ny, nz = out.shape
    half = nz // 2
    y = edge_strip(
        False, own, xm, xp, yp, cm, cp, l1, l2, (w1, w2, w3), bias, s0, s1, s2
    )
    pattern = spread_pattern(half, nz)
    for x in range(nx):
        lines = [low[x, i] for i in range(3)] + [mid[x, i] for i in range(ny - 6)]
        lines += [y[x][i, :half] for i in range(3)]
        for first in range(0, ny, 4):
            r = lax.dot_general(
                jnp.concatenate(lines[first : first + 4], axis=0),
                pattern,
                (((0,), (0,)), ((), ())),
                preferred_element_type=F32,
            )
            r = r[:c, : 4 * nz] + r[c:, 4 * nz :]
            for i in range(4):
                stage[x, pl.ds(first + i, c, stride=ny), :] = r[
                    :, i * nz : (i + 1) * nz
                ]
        out[:, x] = stage[x].reshape(c, ny, nz).astype(BF16)


def shift(x, axis, up):
    count = lax.axis_size(axis)
    pairs = [(i, (i + 1) % count) if up else ((i + 1) % count, i) for i in range(count)]
    return lax.ppermute(x, axis, pairs)


def shards(field, kernel_one, bias_one, kernel_two, bias_two, kernel_three, bias_three):
    h = HALO
    field = field[0]
    c, nx, ny, nz = field.shape
    rows = around((nz + 2 * h) // 2, 8)
    pad = around(rows, 16)
    half = nz // 2
    line = 2 * c

    pairs, edges = call(
        rows_kernel,
        [((nx, ny, rows, line), BF16), ((nx, ny, 4, line), BF16)],
        [pltpu.VMEM((nx, c * ny, nz), F32)],
    )(field)
    if lax.axis_size("gz") == 2:
        edges = shift(edges, "gz", True)
    else:
        edges = jnp.concatenate(
            [shift(edges[:, :, :2], "gz", True), shift(edges[:, :, 2:], "gz", False)],
            axis=2,
        )
    xface = ((h, ny, rows, line), BF16)
    yface = ((nx, h, rows, line), BF16)
    own, xu, xd, yu, yd = call(
        faces_kernel,
        [((nx, ny, rows, line), BF16), xface, xface, yface, yface],
        [pltpu.VMEM((nx, ny, 8, line), F32)],
    )(pairs, edges)
    xm = shift(xu, "gx", True)
    xp = shift(xd, "gx", False)
    ym = shift(yu, "gy", True)
    yp = shift(yd, "gy", False)
    cmm = shift(ym[nx - h :], "gx", True)
    cpm = shift(ym[:h], "gx", False)
    cmp = shift(yp[nx - h :], "gx", True)
    cpp = shift(yp[:h], "gx", False)
    w1, w2, w3, bias = call(
        weights_kernel,
        [((18 * c, 4 * c), BF16)] * 3 + [((3, line), F32)],
        flops=2 * 10**9,
        nbytes=10**6,
    )(
        kernel_one, kernel_two, kernel_three,
        bias_one[None], bias_two[None], bias_three[None],
    )
    (l1,) = call(
        middle_first,
        [((nx + 4, ny - 2, pad, line), BF16)],
        [pltpu.VMEM((nx + 6, ny, pad, line), BF16)],
        flops=3 * 10**9,
        nbytes=10**6,
    )(own, xm, xp, w1, bias)
    l2, l3 = call(
        middle_second,
        [((nx + 2, ny - 4, pad, line), BF16), ((nx, ny - 6, half, line), BF16)],
        flops=2 * 10**9,
        nbytes=10**6,
    )(l1, w2, w3, bias)
    strips = [pltpu.VMEM((nx + k, 5, pad, line), BF16) for k in (6, 4, 2)]
    (low,) = call(
        lower_kernel, [((nx, 3, half, line), BF16)], strips,
        flops=4 * 10**9, nbytes=10**6,
    )(own, xm, xp, ym, cmm, cpm, l1, l2, w1, w2, w3, bias)
    (out,) = call(
        upper_kernel,
        [((c, nx, ny, nz), BF16)],
        strips + [pltpu.VMEM((nx, c * ny, nz), F32)],
        flops=4 * 10**9, nbytes=10**6,
    )(own, xm, xp, yp, cmp, cpp, l1, l2, low, l3, w1, w2, w3, bias)
    return out[None]


def solution(mesh):
    return jax.shard_map(
        shards,
        mesh=mesh,
        in_specs=(P(None, None, "gx", "gy", "gz"), P(), P(), P(), P(), P(), P()),
        out_specs=P(None, None, "gx", "gy", "gz"),
        check_vma=False,
    )
```

```python
import jax
import jax.numpy as jnp
from jax import lax
from jax.experimental import pallas as pl
from jax.experimental.pallas import tpu as pltpu
from jax.sharding import PartitionSpec as P


HALO = 3
SQRT_HALF = 0.7071067811865476
BF16 = jnp.bfloat16
F32 = jnp.float32
VMEM = pl.BlockSpec(memory_space=pltpu.VMEM)


def around(size, step):
    return -(-size // step) * step


def call(kernel, outs, scratch=(), flops=0, nbytes=0):
    outs = [jax.ShapeDtypeStruct(s, d) for s, d in outs]

    def run(*args):
        return pl.pallas_call(
            kernel,
            out_shape=outs,
            in_specs=[VMEM] * len(args),
            out_specs=[VMEM] * len(outs),
            scratch_shapes=list(scratch),
            cost_estimate=pl.CostEstimate(
                flops=flops, bytes_accessed=nbytes, transcendentals=0
            ),
            compiler_params=pltpu.CompilerParams(vmem_limit_bytes=48 * 1024 * 1024),
        )(*args)

    return run


def gelu(u):
    return 0.5 * u * (1.0 + lax.erf(u * SQRT_HALF))


def iota(shape, dim):
    return lax.broadcasted_iota(jnp.int32, shape, dim)


def rows_kernel(field, pairs, edges, xu, xd, planes):
    c, nx, ny, nz = field.shape
    rows = pairs.shape[2]
    h = HALO
    m = iota((rows + 8, 2 * nz), 0)
    j = iota((rows + 8, 2 * nz), 1)
    half = nz // 2
    first = jnp.where(m < rows + 2, m - rows + half, m - rows - 1)
    m = jnp.where(m < rows, m, jnp.where(m < rows + 4, first, -8))
    second = (j >= nz).astype(jnp.int32)
    pick = (j - nz * second == 2 * m - 3 + second).astype(F32).astype(BF16)
    blank = jnp.zeros((c, nz), BF16)
    for x in range(nx):
        planes[x] = field[:, x].astype(F32).reshape(c * ny, nz)
        for y in range(0, ny, 2):
            blocks = []
            for k in range(2):
                b = planes[x, pl.ds(y + k, c, stride=ny), :].astype(BF16)
                blocks.append(jnp.concatenate([b, blank], axis=1))
                blocks.append(jnp.concatenate([blank, b], axis=1))
            r = lax.dot_general(
                pick,
                jnp.concatenate(blocks, axis=0),
                (((1,), (1,)), ((), ())),
                preferred_element_type=F32,
            ).astype(BF16)
            for k in range(2):
                lanes = slice(2 * c * k, 2 * c * (k + 1))
                pairs[x, y + k] = r[:rows, lanes]
                edges[x, y + k] = r[rows : rows + 4, lanes]
                if x >= nx - h:
                    xu[x - nx + h, y + k] = r[:rows, lanes]
                if x < h:
                    xd[x, y + k] = r[:rows, lanes]


def end_rows(lines, edges, wide):
    rows = lines.shape[2]
    wide[:, :, :4] = edges[...].astype(F32)
    got = wide[...]
    row = iota(got.shape, 2)
    low = jnp.where(row < 2, got, 0.0)
    moved = pltpu.roll(got, got.shape[2] - 1, 2)
    high = jnp.where((row >= 1) & (row < 3), moved, 0.0)
    first = lines[:, :, :8].astype(F32) + low
    last = lines[:, :, rows - 8 :].astype(F32) + high
    return first, last


def faces_kernel(pairs, edges, own, yu, yd, eu, ed, wide):
    nx, ny, rows, line = pairs.shape
    h = HALO
    first, last = end_rows(pairs, edges, wide)
    e = jnp.concatenate(
        [first, pairs[:, :, 8 : rows - 8].astype(F32), last], axis=2
    )
    own[...] = e.reshape(nx, ny * rows, line).astype(BF16)
    e = e.astype(BF16)
    yu[...] = e[:, ny - h :]
    yd[...] = e[:, :h]
    eu[...] = edges[nx - h :]
    ed[...] = edges[:h]


def weights_kernel(k1, k2, k3, b1, b2, b3, w1, w2, w3, bias):
    _, _, taps, o, c = k1.shape
    j = iota((taps * o, 8 * o), 0)
    n = iota((taps * o, 8 * o), 1)
    p = n // (4 * o)
    t = n // (2 * o) % 2
    q = n // o % 2
    pick = (j == (p - q + 2 * t) * o + n % o).astype(F32).astype(BF16)
    for k, w in ((k1, w1), (k2, w2), (k3, w3)):
        for a in range(3):
            for e in range(3):
                r = lax.dot_general(
                    k[a, e].reshape(taps * o, c),
                    pick,
                    (((0,), (0,)), ((), ())),
                    preferred_element_type=F32,
                ).astype(BF16)
                at = (a * 3 + e) * 2 * c
                w[at : at + c] = r[:, : 4 * o]
                w[at + c : at + 2 * c] = r[:, 4 * o :]
    for i, b in enumerate((b1, b2, b3)):
        bias[i : i + 1] = jnp.concatenate([b[...], b[...]], axis=1)


def conv(source, x, rows, lines, weight, bias):
    height = around(lines * rows, 16)
    taps = [
        source[x + a, e * rows : e * rows + height] for a in range(3) for e in range(3)
    ]
    both = jnp.dot(jnp.concatenate(taps, axis=1), weight, preferred_element_type=F32)
    u = both[:, :128] + pltpu.roll(both[:, 128:], height - 1, 0) + bias
    return gelu(u).astype(BF16)[: lines * rows]


def middle_own(own, w1, bias, rows, l1):
    lines = own.shape[1] // rows - 2
    for x in range(l1.shape[0]):
        l1[x] = conv(own, x, rows, lines, w1[...], bias[0:1])


def middle_first(own, xm, xp, em, ep, l1own, w1, bias, l1, near, s0, wide):
    h, ny, rows, line = xm.shape
    nx = own.shape[0]
    for at, face, edges in ((0, xm, em), (h + nx, xp, ep)):
        s0[at : at + h] = face[...].reshape(h, ny * rows, line)
        first, last = end_rows(face, edges, wide)
        for i in range(h):
            for y in range(ny):
                s0[at + i, y * rows : y * rows + 8] = first[i, y].astype(BF16)
                s0[at + i, y * rows + rows - 8 : (y + 1) * rows] = last[i, y].astype(
                    BF16
                )
    s0[h : h + nx] = own[...]
    near[:, : 2 * rows] = s0[:, : 2 * rows]
    near[:, 2 * rows :] = s0[:, (ny - 2) * rows :]
    for x in range(nx + 4):
        if 3 <= x < nx + 1:
            l1[x] = l1own[x - 3]
        else:
            l1[x] = conv(s0, x, rows, ny - 2, w1[...], bias[0:1])


def middle_second(l1, w2, w3, bias, rows, l2, l3):
    lines = l1.shape[1] // rows - 2
    half = l3.shape[2]
    for x in range(l2.shape[0]):
        l2[x] = conv(l1, x, rows, lines, w2[...], bias[1:2])
    for x in range(l3.shape[0]):
        y = conv(l2, x, rows, lines - 2, w3[...], bias[2:3])
        for i in range(lines - 2):
            l3[x, i] = y[i * rows : i * rows + half]


def spread_pattern(half, nz):
    r = iota((4 * half, 8 * nz), 0)
    n = iota((4 * half, 8 * nz), 1)
    hit = (r // half == n // nz % 4) & (n % nz == 2 * (r % half) + n // (4 * nz))
    return hit.astype(F32).astype(BF16)


def edge_strip(below, near, side, cm, cp, l1, l2, ws, bias, s0, s1, s2):
    nx, h, rows, line = side.shape
    close = slice(3 * rows, 5 * rows) if below else slice(0, 2 * rows)
    far = slice(0, 3 * rows) if below else slice(2 * rows, 5 * rows)
    part = slice(0, 2 * rows) if below else slice(2 * rows, 4 * rows)
    end1 = part if below else slice(l1.shape[1] - 2 * rows, l1.shape[1])
    end2 = part if below else slice(l2.shape[1] - 2 * rows, l2.shape[1])
    s0[:, close] = near[:, part]
    s0[:h, far] = cm[...].reshape(h, h * rows, line)
    s0[h : h + nx, far] = side[...].reshape(nx, h * rows, line)
    s0[h + nx :, far] = cp[...].reshape(h, h * rows, line)
    s1[:, close] = l1[:, end1]
    s2[:, close] = l2[:, end2]
    for source, target, i in ((s0, s1, 0), (s1, s2, 1)):
        for x in range(source.shape[0] - 2):
            target[x, far] = conv(source, x, rows, 3, ws[i][...], bias[i : i + 1])
    return [conv(s2, x, rows, 3, ws[2][...], bias[2:3]) for x in range(nx)]


def lower_kernel(near, ym, cm, cp, l1, l2, w1, w2, w3, bias, low, s0, s1, s2):
    rows = ym.shape[2]
    half = low.shape[2]
    y = edge_strip(True, near, ym, cm, cp, l1, l2, (w1, w2, w3), bias, s0, s1, s2)
    for x, lines in enumerate(y):
        for i in range(3):
            low[x, i] = lines[i * rows : i * rows + half]


def upper_kernel(
    near, yp, cm, cp, l1, l2, low, mid, w1, w2, w3, bias, out, s0, s1, s2, stage
):
    c, nx, ny, nz = out.shape
    rows = yp.shape[2]
    half = nz // 2
    y = edge_strip(False, near, yp, cm, cp, l1, l2, (w1, w2, w3), bias, s0, s1, s2)
    pattern = spread_pattern(half, nz)
    for x in range(nx):
        lines = [low[x, i] for i in range(3)] + [mid[x, i] for i in range(ny - 6)]
        lines += [y[x][i * rows : i * rows + half] for i in range(3)]
        for first in range(0, ny, 4):
            r = lax.dot_general(
                jnp.concatenate(lines[first : first + 4], axis=0),
                pattern,
                (((0,), (0,)), ((), ())),
                preferred_element_type=F32,
            )
            r = r[:c, : 4 * nz] + r[c:, 4 * nz :]
            for i in range(4):
                stage[x, pl.ds(first + i, c, stride=ny), :] = r[
                    :, i * nz : (i + 1) * nz
                ]
        out[:, x] = stage[x].reshape(c, ny, nz).astype(BF16)


def shift(x, axis, up):
    count = lax.axis_size(axis)
    pairs = [(i, (i + 1) % count) if up else ((i + 1) % count, i) for i in range(count)]
    return lax.ppermute(x, axis, pairs)


def shards(field, kernel_one, bias_one, kernel_two, bias_two, kernel_three, bias_three):
    h = HALO
    field = field[0]
    c, nx, ny, nz = field.shape
    rows = around((nz + 2 * h) // 2, 8)
    half = nz // 2
    line = 2 * c

    xface = ((h, ny, rows, line), BF16)
    yface = ((nx, h, rows, line), BF16)
    pairs, edges, xu, xd = call(
        rows_kernel,
        [((nx, ny, rows, line), BF16), ((nx, ny, 4, line), BF16), xface, xface],
        [pltpu.VMEM((nx, c * ny, nz), F32)],
    )(field)
    if lax.axis_size("gz") == 2:
        edges = shift(edges, "gz", True)
    else:
        edges = jnp.concatenate(
            [shift(edges[:, :, :2], "gz", True), shift(edges[:, :, 2:], "gz", False)],
            axis=2,
        )
    xm = shift(xu, "gx", True)
    xp = shift(xd, "gx", False)
    own, yu, yd, eu, ed = call(
        faces_kernel,
        [
            ((nx, ny * rows, line), BF16), yface, yface,
            ((h, ny, 4, line), BF16), ((h, ny, 4, line), BF16),
        ],
        [pltpu.VMEM((nx, ny, 8, line), F32)],
    )(pairs, edges)
    em = shift(eu, "gx", True)
    ep = shift(ed, "gx", False)
    ym = shift(yu, "gy", True)
    yp = shift(yd, "gy", False)
    cmm = shift(ym[nx - h :], "gx", True)
    cpm = shift(ym[:h], "gx", False)
    cmp = shift(yp[nx - h :], "gx", True)
    cpp = shift(yp[:h], "gx", False)
    w1, w2, w3, bias = call(
        weights_kernel,
        [((18 * c, 4 * c), BF16)] * 3 + [((3, line), F32)],
        flops=2 * 10**9,
        nbytes=10**6,
    )(
        kernel_one, kernel_two, kernel_three,
        bias_one[None], bias_two[None], bias_three[None],
    )
    (l1own,) = call(
        lambda o, w, b, l: middle_own(o, w, b, rows, l),
        [((nx - 2, (ny - 2) * rows, line), BF16)],
        flops=10**9,
        nbytes=10**6,
    )(own, w1, bias)
    l1, near = call(
        middle_first,
        [
            ((nx + 4, (ny - 2) * rows, line), BF16),
            ((nx + 6, 4 * rows, line), BF16),
        ],
        [
            pltpu.VMEM((nx + 6, ny * rows, line), BF16),
            pltpu.VMEM((h, ny, 8, line), F32),
        ],
        flops=2 * 10**9,
        nbytes=10**6,
    )(own, xm, xp, em, ep, l1own, w1, bias)
    l2, l3 = call(
        lambda a, v, w, b, o, p: middle_second(a, v, w, b, rows, o, p),
        [
            ((nx + 2, (ny - 4) * rows, line), BF16),
            ((nx, ny - 6, half, line), BF16),
        ],
        flops=2 * 10**9,
        nbytes=10**6,
    )(l1, w2, w3, bias)
    deep = around(3 * rows, 16) + 2 * rows
    strips = [pltpu.VMEM((nx + k, deep, line), BF16) for k in (6, 4, 2)]
    (low,) = call(
        lower_kernel, [((nx, 3, half, line), BF16)], strips,
        flops=4 * 10**9, nbytes=10**6,
    )(near, ym, cmm, cpm, l1, l2, w1, w2, w3, bias)
    (out,) = call(
        upper_kernel,
        [((c, nx, ny, nz), BF16)],
        strips + [pltpu.VMEM((nx, c * ny, nz), F32)],
        flops=4 * 10**9, nbytes=10**6,
    )(near, yp, cmp, cpp, l1, l2, low, l3, w1, w2, w3, bias)
    return out[None]


def solution(mesh):
    return jax.shard_map(
        shards,
        mesh=mesh,
        in_specs=(P(None, None, "gx", "gy", "gz"), P(), P(), P(), P(), P(), P()),
        out_specs=P(None, None, "gx", "gy", "gz"),
        check_vma=False,
    )
```

```python
import jax
import jax.numpy as jnp
from jax import lax
from jax.experimental import pallas as pl
from jax.experimental.pallas import tpu as pltpu
from jax.sharding import PartitionSpec as P


HALO = 3
SQRT_HALF = 0.7071067811865476
BF16 = jnp.bfloat16
F32 = jnp.float32
VMEM = pl.BlockSpec(memory_space=pltpu.VMEM)


def around(size, step):
    return -(-size // step) * step


def call(kernel, outs, scratch=(), flops=0, nbytes=0, far=0):
    outs = [jax.ShapeDtypeStruct(s, d) for s, d in outs]

    def run(*args):
        args = list(args)
        for i in range(len(args) - far, len(args)):
            args[i] = pltpu.with_memory_space_constraint(args[i], pltpu.HBM)
        return pl.pallas_call(
            kernel,
            out_shape=outs,
            in_specs=[VMEM] * (len(args) - far)
            + [pl.BlockSpec(memory_space=pltpu.HBM)] * far,
            out_specs=[VMEM] * len(outs),
            scratch_shapes=list(scratch),
            cost_estimate=pl.CostEstimate(
                flops=flops, bytes_accessed=nbytes, transcendentals=0
            ),
            compiler_params=pltpu.CompilerParams(vmem_limit_bytes=24 * 1024 * 1024),
        )(*args)

    return run


def gelu(u):
    return 0.5 * u * (1.0 + lax.erf(u * SQRT_HALF))


def iota(shape, dim):
    return lax.broadcasted_iota(jnp.int32, shape, dim)


def is_even(axis):
    return lax.rem(lax.axis_index(axis), 2) == 0


def rows_kernel(field, pairs, edges, xu, xd, planes):
    c, nx, ny, nz = field.shape
    rows = pairs.shape[2]
    h = HALO
    m = iota((rows + 8, 2 * nz), 0)
    j = iota((rows + 8, 2 * nz), 1)
    half = nz // 2
    first = jnp.where(m < rows + 2, m - rows + half, m - rows - 1)
    m = jnp.where(m < rows, m, jnp.where(m < rows + 4, first, -8))
    second = (j >= nz).astype(jnp.int32)
    pick = (j - nz * second == 2 * m - 3 + second).astype(F32).astype(BF16)
    blank = jnp.zeros((c, nz), BF16)
    for x in range(nx):
        planes[x] = field[:, x].astype(F32).reshape(c * ny, nz)
        for y in range(0, ny, 2):
            blocks = []
            for k in range(2):
                b = planes[x, pl.ds(y + k, c, stride=ny), :].astype(BF16)
                blocks.append(jnp.concatenate([b, blank], axis=1))
                blocks.append(jnp.concatenate([blank, b], axis=1))
            r = lax.dot_general(
                pick,
                jnp.concatenate(blocks, axis=0),
                (((1,), (1,)), ((), ())),
                preferred_element_type=F32,
            ).astype(BF16)
            for k in range(2):
                lanes = slice(2 * c * k, 2 * c * (k + 1))
                pairs[x, y + k] = r[:rows, lanes]
                edges[x, y + k] = r[rows : rows + 4, lanes]
                if x >= nx - h:
                    xu[x - nx + h, y + k] = r[:rows, lanes]
                if x < h:
                    xd[x, y + k] = r[:rows, lanes]


def end_rows(lines, edges, wide):
    rows = lines.shape[2]
    wide[:, :, :4] = edges[...].astype(F32)
    got = wide[...]
    row = iota(got.shape, 2)
    low = jnp.where(row < 2, got, 0.0)
    moved = pltpu.roll(got, got.shape[2] - 1, 2)
    high = jnp.where((row >= 1) & (row < 3), moved, 0.0)
    first = lines[:, :, :8].astype(F32) + low
    last = lines[:, :, rows - 8 :].astype(F32) + high
    return first, last


def faces_kernel(pairs, edges, own, ya, yb, eu, ed, wide):
    nx, ny, rows, line = pairs.shape
    h = HALO
    first, last = end_rows(pairs, edges, wide)
    e = jnp.concatenate(
        [first, pairs[:, :, 8 : rows - 8].astype(F32), last], axis=2
    )
    own[...] = e.reshape(nx, ny * rows, line).astype(BF16)
    e = e.astype(BF16)
    even = is_even("gy")
    head, tail = e[:, :h], e[:, ny - h :]

    @pl.when(even)
    def _():
        ya[...] = tail
        yb[...] = head

    @pl.when(jnp.logical_not(even))
    def _():
        ya[...] = head
        yb[...] = tail

    eu[...] = edges[nx - h :]
    ed[...] = edges[:h]


def weights_kernel(
    k1, k2, k3, b1, b2, b3, w1, w2, w3, bias, pattern, thin, sems
):
    _, _, taps, o, c = k1.shape
    copies = [
        pltpu.make_async_copy(b, thin.at[i], sems.at[i])
        for i, b in enumerate((b1, b2, b3))
    ]
    for copy in copies:
        copy.start()
    nz = pattern.shape[1] // 4
    pattern[...] = spread_pattern(nz // 2, nz)
    j = iota((taps * o, 8 * o), 0)
    n = iota((taps * o, 8 * o), 1)
    p = n // (4 * o)
    t = n // (2 * o) % 2
    q = n // o % 2
    pick = (j == (p - q + 2 * t) * o + n % o).astype(F32).astype(BF16)
    for k, w in ((k1, w1), (k2, w2), (k3, w3)):
        for a in range(3):
            for e in range(3):
                r = lax.dot_general(
                    k[a, e].reshape(taps * o, c),
                    pick,
                    (((0,), (0,)), ((), ())),
                    preferred_element_type=F32,
                ).astype(BF16)
                at = (a * 3 + e) * 2 * c
                w[at : at + c] = r[:, : 4 * o]
                w[at + c : at + 2 * c] = r[:, 4 * o :]
    for copy in copies:
        copy.wait()
    for i in range(3):
        bias[i : i + 1] = jnp.concatenate([thin[i], thin[i]], axis=1)


def conv(source, x, rows, lines, weight, bias):
    height = around(lines * rows, 16)
    taps = [
        source[x + a, e * rows : e * rows + height] for a in range(3) for e in range(3)
    ]
    both = jnp.dot(jnp.concatenate(taps, axis=1), weight, preferred_element_type=F32)
    u = both[:, :128] + pltpu.roll(both[:, 128:], height - 1, 0) + bias
    return gelu(u).astype(BF16)[: lines * rows]


def middle_own(own, w1, bias, rows, l1):
    lines = own.shape[1] // rows - 2
    for x in range(l1.shape[0]):
        l1[x] = conv(own, x, rows, lines, w1[...], bias[0:1])


def middle_first(own, xm, xp, em, ep, l1own, w1, bias, l1, near, s0, wide):
    h, ny, rows, line = xm.shape
    nx = own.shape[0]
    for at, face, edges in ((0, xm, em), (h + nx, xp, ep)):
        s0[at : at + h] = face[...].reshape(h, ny * rows, line)
        first, last = end_rows(face, edges, wide)
        for i in range(h):
            for y in range(ny):
                s0[at + i, y * rows : y * rows + 8] = first[i, y].astype(BF16)
                s0[at + i, y * rows + rows - 8 : (y + 1) * rows] = last[i, y].astype(
                    BF16
                )
    s0[h : h + nx] = own[...]
    near[:, : 2 * rows] = s0[:, : 2 * rows]
    near[:, 2 * rows :] = s0[:, (ny - 2) * rows :]
    for x in range(nx + 4):
        if 3 <= x < nx + 1:
            l1[x] = l1own[x - 3]
        else:
            l1[x] = conv(s0, x, rows, ny - 2, w1[...], bias[0:1])


def middle_second(l1, w2, w3, bias, rows, l2, l3):
    lines = l1.shape[1] // rows - 2
    half = l3.shape[2]
    for x in range(l2.shape[0]):
        l2[x] = conv(l1, x, rows, lines, w2[...], bias[1:2])
    for x in range(l3.shape[0]):
        y = conv(l2, x, rows, lines - 2, w3[...], bias[2:3])
        for i in range(lines - 2):
            l3[x, i] = y[i * rows : i * rows + half]


def spread_pattern(half, nz):
    r = iota((8 * half, 4 * nz), 0)
    n = iota((8 * half, 4 * nz), 1)
    line = r // half % 4
    hit = (line == n // nz) & (n % nz == 2 * (r % half) + r // (4 * half))
    return hit.astype(F32).astype(BF16)


def edge_strip(below, near, side, ca, cb, l1, l2, ws, bias, s0, s1, s2):
    nx, h, rows, line = side.shape
    close = slice(3 * rows, 5 * rows) if below else slice(0, 2 * rows)
    far = slice(0, 3 * rows) if below else slice(2 * rows, 5 * rows)
    part = slice(0, 2 * rows) if below else slice(2 * rows, 4 * rows)
    end1 = part if below else slice(l1.shape[1] - 2 * rows, l1.shape[1])
    end2 = part if below else slice(l2.shape[1] - 2 * rows, l2.shape[1])
    first = jnp.where(is_even("gx"), h + nx, 0)
    s0[:, close] = near[:, part]
    s0[pl.ds(first, h), far] = ca[...].reshape(h, h * rows, line)
    s0[pl.ds(h + nx - first, h), far] = cb[...].reshape(h, h * rows, line)
    s0[h : h + nx, far] = side[...].reshape(nx, h * rows, line)
    s1[:, close] = l1[:, end1]
    s2[:, close] = l2[:, end2]
    for source, target, i in ((s0, s1, 0), (s1, s2, 1)):
        for x in range(source.shape[0] - 2):
            target[x, far] = conv(source, x, rows, 3, ws[i][...], bias[i : i + 1])
    return [conv(s2, x, rows, 3, ws[2][...], bias[2:3]) for x in range(nx)]


def by_side(even_below, body):
    even = is_even("gy")

    @pl.when(even)
    def _():
        body(even_below)

    @pl.when(jnp.logical_not(even))
    def _():
        body(not even_below)


def first_kernel(near, side, ca, cb, l1, l2, w1, w2, w3, bias, out, s0, s1, s2):
    rows = side.shape[2]
    half = out.shape[2]

    def body(below):
        ws = (w1, w2, w3)
        y = edge_strip(below, near, side, ca, cb, l1, l2, ws, bias, s0, s1, s2)
        for x, lines in enumerate(y):
            for i in range(3):
                out[x, i] = lines[i * rows : i * rows + half]

    by_side(False, body)


def second_kernel(
    near, side, ca, cb, l1, l2, other, mid, w1, w2, w3, bias, pattern, out,
    s0, s1, s2, stage,
):
    c, nx, ny, nz = out.shape
    rows = side.shape[2]
    half = nz // 2

    def body(below):
        ws = (w1, w2, w3)
        y = edge_strip(below, near, side, ca, cb, l1, l2, ws, bias, s0, s1, s2)
        for x in range(nx):
            mine = [y[x][i * rows : i * rows + half] for i in range(3)]
            theirs = [other[x, i] for i in range(3)]
            inner = [mid[x, i] for i in range(ny - 6)]
            lines = mine + inner + theirs if below else theirs + inner + mine
            parts = [
                jnp.concatenate(lines[first : first + 4], axis=0)
                for first in range(0, ny, 4)
            ]
            sides = [
                jnp.concatenate([p[:, q * c : (q + 1) * c] for p in parts], axis=1)
                for q in range(2)
            ]
            r = lax.dot_general(
                jnp.concatenate(sides, axis=0),
                pattern[...],
                (((0,), (0,)), ((), ())),
                preferred_element_type=F32,
            )
            for i in range(ny):
                stage[x, pl.ds(i, c, stride=ny), :] = r[
                    i // 4 * c : (i // 4 + 1) * c, i % 4 * nz : (i % 4 + 1) * nz
                ]
            out[:, x] = stage[x].reshape(c, ny, nz).astype(BF16)

    by_side(True, body)


def shift(x, axis, up):
    count = lax.axis_size(axis)
    pairs = [(i, (i + 1) % count) if up else ((i + 1) % count, i) for i in range(count)]
    return lax.ppermute(x, axis, pairs)


def swap(x, axis, first):
    count = lax.axis_size(axis)
    assert count % 2 == 0
    up = 1 if first else -1
    pairs = [(i, (i + (up if i % 2 == 0 else -up)) % count) for i in range(count)]
    return lax.ppermute(x, axis, pairs)


def shards(field, kernel_one, bias_one, kernel_two, bias_two, kernel_three, bias_three):
    h = HALO
    field = field[0]
    c, nx, ny, nz = field.shape
    rows = around((nz + 2 * h) // 2, 8)
    half = nz // 2
    line = 2 * c

    xface = ((h, ny, rows, line), BF16)
    yface = ((nx, h, rows, line), BF16)
    pairs, edges, xu, xd = call(
        rows_kernel,
        [((nx, ny, rows, line), BF16), ((nx, ny, 4, line), BF16), xface, xface],
        [pltpu.VMEM((nx, c * ny, nz), F32)],
        flops=8 * 10**9,
        nbytes=10**6,
    )(field)
    if lax.axis_size("gz") == 2:
        edges = shift(edges, "gz", True)
    else:
        edges = jnp.concatenate(
            [shift(edges[:, :, :2], "gz", True), shift(edges[:, :, 2:], "gz", False)],
            axis=2,
        )
    xm = shift(xu, "gx", True)
    xp = shift(xd, "gx", False)
    parameters = (
        kernel_one, kernel_two, kernel_three,
        bias_one[None], bias_two[None], bias_three[None],
    )
    own, ya, yb, eu, ed = call(
        faces_kernel,
        [
            ((nx, ny * rows, line), BF16), yface, yface,
            ((h, ny, 4, line), BF16), ((h, ny, 4, line), BF16),
        ],
        [pltpu.VMEM((nx, ny, 8, line), F32)],
        flops=8 * 10**9,
        nbytes=10**6,
    )(pairs, edges)
    em = shift(eu, "gx", True)
    ep = shift(ed, "gx", False)
    ya = swap(ya, "gy", True)
    yb = swap(yb, "gy", False)
    tail = jnp.where(is_even("gx"), nx - h, 0)

    def planes(side, start):
        return lax.dynamic_slice_in_dim(side, start, h, axis=0)

    caa = swap(planes(ya, tail), "gx", True)
    cab = swap(planes(ya, nx - h - tail), "gx", False)
    cba = swap(planes(yb, tail), "gx", True)
    cbb = swap(planes(yb, nx - h - tail), "gx", False)
    w1, w2, w3, bias, pattern = call(
        weights_kernel,
        [((18 * c, 4 * c), BF16)] * 3
        + [((3, line), F32), ((4 * nz, 4 * nz), BF16)],
        [pltpu.VMEM((3, 1, c), F32), pltpu.SemaphoreType.DMA((3,))],
        far=3,
        flops=2 * 10**9,
        nbytes=10**6,
    )(*parameters)
    (l1own,) = call(
        lambda o, w, b, l: middle_own(o, w, b, rows, l),
        [((nx - 2, (ny - 2) * rows, line), BF16)],
        flops=10**9,
        nbytes=10**6,
    )(own, w1, bias)
    l1, near = call(
        middle_first,
        [
            ((nx + 4, (ny - 2) * rows, line), BF16),
            ((nx + 6, 4 * rows, line), BF16),
        ],
        [
            pltpu.VMEM((nx + 6, ny * rows, line), BF16),
            pltpu.VMEM((h, ny, 8, line), F32),
        ],
        flops=2 * 10**9,
        nbytes=10**6,
    )(own, xm, xp, em, ep, l1own, w1, bias)
    l2, l3 = call(
        lambda a, v, w, b, o, p: middle_second(a, v, w, b, rows, o, p),
        [
            ((nx + 2, (ny - 4) * rows, line), BF16),
            ((nx, ny - 6, half, line), BF16),
        ],
        flops=2 * 10**9,
        nbytes=10**6,
    )(l1, w2, w3, bias)
    deep = around(3 * rows, 16) + 2 * rows
    strips = [pltpu.VMEM((nx + k, deep, line), BF16) for k in (6, 4, 2)]
    (strip,) = call(
        first_kernel, [((nx, 3, half, line), BF16)], strips,
        flops=4 * 10**9, nbytes=10**6,
    )(near, ya, caa, cab, l1, l2, w1, w2, w3, bias)
    (out,) = call(
        second_kernel,
        [((c, nx, ny, nz), BF16)],
        strips + [pltpu.VMEM((nx, c * ny, nz), F32)],
        flops=4 * 10**9, nbytes=10**6,
    )(near, yb, cba, cbb, l1, l2, strip, l3, w1, w2, w3, bias, pattern)
    return out[None]


def solution(mesh):
    return jax.shard_map(
        shards,
        mesh=mesh,
        in_specs=(P(None, None, "gx", "gy", "gz"), P(), P(), P(), P(), P(), P()),
        out_specs=P(None, None, "gx", "gy", "gz"),
        check_vma=False,
    )
```

```python
import jax
import jax.numpy as jnp
from jax import lax
from jax.experimental import pallas as pl
from jax.experimental.pallas import tpu as pltpu
from jax.sharding import PartitionSpec as P


HALO = 3
SQRT_HALF = 0.7071067811865476
BF16 = jnp.bfloat16
F32 = jnp.float32
VMEM = pl.BlockSpec(memory_space=pltpu.VMEM)


def around(size, step):
    return -(-size // step) * step


def call(kernel, outs, scratch=(), flops=0, nbytes=0, far=0):
    outs = [jax.ShapeDtypeStruct(s, d) for s, d in outs]

    def run(*args):
        args = list(args)
        for i in range(len(args) - far, len(args)):
            args[i] = pltpu.with_memory_space_constraint(args[i], pltpu.HBM)
        return pl.pallas_call(
            kernel,
            out_shape=outs,
            in_specs=[VMEM] * (len(args) - far)
            + [pl.BlockSpec(memory_space=pltpu.HBM)] * far,
            out_specs=[VMEM] * len(outs),
            scratch_shapes=list(scratch),
            cost_estimate=pl.CostEstimate(
                flops=flops, bytes_accessed=nbytes, transcendentals=0
            ),
            compiler_params=pltpu.CompilerParams(vmem_limit_bytes=24 * 1024 * 1024),
        )(*args)

    return run


def gelu(u):
    return 0.5 * u * (1.0 + lax.erf(u * SQRT_HALF))


def iota(shape, dim):
    return lax.broadcasted_iota(jnp.int32, shape, dim)


def is_even(axis):
    return lax.rem(lax.axis_index(axis), 2) == 0


def rows_kernel(field, pairs, edges, xu, xd, planes):
    c, nx, ny, nz = field.shape
    rows = pairs.shape[2]
    h = HALO
    tall = rows + 8
    m = iota((2 * tall, nz), 0)
    second = (m >= tall).astype(jnp.int32)
    m = m - tall * second
    half = nz // 2
    first = jnp.where(m < rows + 2, m - rows + half, m - rows - 1)
    m = jnp.where(m < rows, m, jnp.where(m < rows + 4, first, -8))
    pick = (iota((2 * tall, nz), 1) == 2 * m - 3 + second).astype(F32).astype(BF16)
    for x in range(nx):
        planes[x] = field[:, x].astype(F32).reshape(c * ny, nz)
        for y in range(0, ny, 4):
            lines = [
                planes[x, pl.ds(y + k, c, stride=ny), :].astype(BF16) for k in range(4)
            ]
            r = lax.dot_general(
                pick,
                jnp.concatenate(lines, axis=0),
                (((1,), (1,)), ((), ())),
                preferred_element_type=F32,
            ).astype(BF16)
            for k in range(4):
                lanes = slice(c * k, c * (k + 1))
                line = jnp.concatenate([r[:tall, lanes], r[tall:, lanes]], axis=1)
                pairs[x, y + k] = line[:rows]
                edges[x, y + k] = line[rows : rows + 4]
                if x >= nx - h:
                    xu[x - nx + h, y + k] = line[:rows]
                if x < h:
                    xd[x, y + k] = line[:rows]


def end_rows(lines, edges, wide):
    rows = lines.shape[2]
    wide[:, :, :4] = edges[...].astype(F32)
    got = wide[...]
    row = iota(got.shape, 2)
    low = jnp.where(row < 2, got, 0.0)
    moved = pltpu.roll(got, got.shape[2] - 1, 2)
    high = jnp.where((row >= 1) & (row < 3), moved, 0.0)
    first = lines[:, :, :8].astype(F32) + low
    last = lines[:, :, rows - 8 :].astype(F32) + high
    return first, last


def faces_kernel(pairs, edges, own, ya, yb, eu, ed, wide):
    nx, ny, rows, line = pairs.shape
    h = HALO
    first, last = end_rows(pairs, edges, wide)
    e = jnp.concatenate(
        [first, pairs[:, :, 8 : rows - 8].astype(F32), last], axis=2
    )
    own[...] = e.reshape(nx, ny * rows, line).astype(BF16)
    e = e.astype(BF16)
    even = is_even("gy")
    head, tail = e[:, :h], e[:, ny - h :]

    @pl.when(even)
    def _():
        ya[...] = tail
        yb[...] = head

    @pl.when(jnp.logical_not(even))
    def _():
        ya[...] = head
        yb[...] = tail

    eu[...] = edges[nx - h :]
    ed[...] = edges[:h]


def weights_kernel(
    k1, k2, k3, b1, b2, b3, w1, w2, w3, bias, pattern, thin, sems
):
    _, _, taps, o, c = k1.shape
    copies = [
        pltpu.make_async_copy(b, thin.at[i], sems.at[i])
        for i, b in enumerate((b1, b2, b3))
    ]
    for copy in copies:
        copy.start()
    nz = pattern.shape[1] // 4
    pattern[...] = spread_pattern(nz // 2, nz)
    j = iota((taps * o, 8 * o), 0)
    n = iota((taps * o, 8 * o), 1)
    p = n // (4 * o)
    t = n // (2 * o) % 2
    q = n // o % 2
    pick = (j == (p - q + 2 * t) * o + n % o).astype(F32).astype(BF16)
    for k, w in ((k1, w1), (k2, w2), (k3, w3)):
        for a in range(3):
            for e in range(3):
                r = lax.dot_general(
                    k[a, e].reshape(taps * o, c),
                    pick,
                    (((0,), (0,)), ((), ())),
                    preferred_element_type=F32,
                ).astype(BF16)
                at = (a * 3 + e) * 2 * c
                w[at : at + c] = r[:, : 4 * o]
                w[at + c : at + 2 * c] = r[:, 4 * o :]
    for copy in copies:
        copy.wait()
    for i in range(3):
        bias[i : i + 1] = jnp.concatenate([thin[i], thin[i]], axis=1)


def conv(source, x, rows, lines, weight, bias):
    height = around(lines * rows, 16)
    taps = [
        source[x + a, e * rows : e * rows + height] for a in range(3) for e in range(3)
    ]
    both = jnp.dot(jnp.concatenate(taps, axis=1), weight, preferred_element_type=F32)
    u = both[:, :128] + pltpu.roll(both[:, 128:], height - 1, 0) + bias
    return gelu(u).astype(BF16)[: lines * rows]


def middle_own(own, w1, bias, rows, l1):
    lines = own.shape[1] // rows - 2
    for x in range(l1.shape[0]):
        l1[x] = conv(own, x, rows, lines, w1[...], bias[0:1])


def middle_first(own, xm, xp, em, ep, l1own, w1, bias, l1, near, s0, wide):
    h, ny, rows, line = xm.shape
    nx = own.shape[0]
    for at, face, edges in ((0, xm, em), (h + nx, xp, ep)):
        s0[at : at + h] = face[...].reshape(h, ny * rows, line)
        first, last = end_rows(face, edges, wide)
        for i in range(h):
            for y in range(ny):
                s0[at + i, y * rows : y * rows + 8] = first[i, y].astype(BF16)
                s0[at + i, y * rows + rows - 8 : (y + 1) * rows] = last[i, y].astype(
                    BF16
                )
    s0[h : h + nx] = own[...]
    near[:, : 2 * rows] = s0[:, : 2 * rows]
    near[:, 2 * rows :] = s0[:, (ny - 2) * rows :]
    for x in range(nx + 4):
        if 3 <= x < nx + 1:
            l1[x] = l1own[x - 3]
        else:
            l1[x] = conv(s0, x, rows, ny - 2, w1[...], bias[0:1])


def middle_second(l1, w2, w3, bias, rows, l2, l3):
    lines = l1.shape[1] // rows - 2
    half = l3.shape[2]
    for x in range(l2.shape[0]):
        l2[x] = conv(l1, x, rows, lines, w2[...], bias[1:2])
    for x in range(l3.shape[0]):
        y = conv(l2, x, rows, lines - 2, w3[...], bias[2:3])
        for i in range(lines - 2):
            l3[x, i] = y[i * rows : i * rows + half]


def spread_pattern(half, nz):
    r = iota((8 * half, 4 * nz), 0)
    n = iota((8 * half, 4 * nz), 1)
    line = r // half % 4
    hit = (line == n // nz) & (n % nz == 2 * (r % half) + r // (4 * half))
    return hit.astype(F32).astype(BF16)


def edge_strip(below, near, side, ca, cb, l1, l2, ws, bias, s0, s1, s2):
    nx, h, rows, line = side.shape
    close = slice(3 * rows, 5 * rows) if below else slice(0, 2 * rows)
    far = slice(0, 3 * rows) if below else slice(2 * rows, 5 * rows)
    part = slice(0, 2 * rows) if below else slice(2 * rows, 4 * rows)
    end1 = part if below else slice(l1.shape[1] - 2 * rows, l1.shape[1])
    end2 = part if below else slice(l2.shape[1] - 2 * rows, l2.shape[1])
    first = jnp.where(is_even("gx"), h + nx, 0)
    s0[:, close] = near[:, part]
    s0[pl.ds(first, h), far] = ca[...].reshape(h, h * rows, line)
    s0[pl.ds(h + nx - first, h), far] = cb[...].reshape(h, h * rows, line)
    s0[h : h + nx, far] = side[...].reshape(nx, h * rows, line)
    s1[:, close] = l1[:, end1]
    s2[:, close] = l2[:, end2]
    for source, target, i in ((s0, s1, 0), (s1, s2, 1)):
        for x in range(source.shape[0] - 2):
            target[x, far] = conv(source, x, rows, 3, ws[i][...], bias[i : i + 1])
    return [conv(s2, x, rows, 3, ws[2][...], bias[2:3]) for x in range(nx)]


def by_side(even_below, body):
    even = is_even("gy")

    @pl.when(even)
    def _():
        body(even_below)

    @pl.when(jnp.logical_not(even))
    def _():
        body(not even_below)


def first_kernel(near, side, ca, cb, l1, l2, w1, w2, w3, bias, out, s0, s1, s2):
    rows = side.shape[2]
    half = out.shape[2]

    def body(below):
        ws = (w1, w2, w3)
        y = edge_strip(below, near, side, ca, cb, l1, l2, ws, bias, s0, s1, s2)
        for x, lines in enumerate(y):
            for i in range(3):
                out[x, i] = lines[i * rows : i * rows + half]

    by_side(False, body)


def second_kernel(
    near, side, ca, cb, l1, l2, other, mid, w1, w2, w3, bias, pattern, out,
    s0, s1, s2, stage,
):
    c, nx, ny, nz = out.shape
    rows = side.shape[2]
    half = nz // 2

    def body(below):
        ws = (w1, w2, w3)
        y = edge_strip(below, near, side, ca, cb, l1, l2, ws, bias, s0, s1, s2)
        for x in range(nx):
            mine = [y[x][i * rows : i * rows + half] for i in range(3)]
            theirs = [other[x, i] for i in range(3)]
            inner = [mid[x, i] for i in range(ny - 6)]
            lines = mine + inner + theirs if below else theirs + inner + mine
            parts = [
                jnp.concatenate(lines[first : first + 4], axis=0)
                for first in range(0, ny, 4)
            ]
            sides = [
                jnp.concatenate([p[:, q * c : (q + 1) * c] for p in parts], axis=1)
                for q in range(2)
            ]
            r = lax.dot_general(
                jnp.concatenate(sides, axis=0),
                pattern[...],
                (((0,), (0,)), ((), ())),
                preferred_element_type=F32,
            )
            for i in range(ny):
                stage[x, pl.ds(i, c, stride=ny), :] = r[
                    i // 4 * c : (i // 4 + 1) * c, i % 4 * nz : (i % 4 + 1) * nz
                ]
            out[:, x] = stage[x].reshape(c, ny, nz).astype(BF16)

    by_side(True, body)


def shift(x, axis, up):
    count = lax.axis_size(axis)
    pairs = [(i, (i + 1) % count) if up else ((i + 1) % count, i) for i in range(count)]
    return lax.ppermute(x, axis, pairs)


def swap(x, axis, first):
    count = lax.axis_size(axis)
    assert count % 2 == 0
    up = 1 if first else -1
    pairs = [(i, (i + (up if i % 2 == 0 else -up)) % count) for i in range(count)]
    return lax.ppermute(x, axis, pairs)


def shards(field, kernel_one, bias_one, kernel_two, bias_two, kernel_three, bias_three):
    h = HALO
    field = field[0]
    c, nx, ny, nz = field.shape
    rows = around((nz + 2 * h) // 2, 8)
    half = nz // 2
    line = 2 * c

    xface = ((h, ny, rows, line), BF16)
    yface = ((nx, h, rows, line), BF16)
    pairs, edges, xu, xd = call(
        rows_kernel,
        [((nx, ny, rows, line), BF16), ((nx, ny, 4, line), BF16), xface, xface],
        [pltpu.VMEM((nx, c * ny, nz), F32)],
        flops=8 * 10**9,
        nbytes=10**6,
    )(field)
    if lax.axis_size("gz") == 2:
        edges = shift(edges, "gz", True)
    else:
        edges = jnp.concatenate(
            [shift(edges[:, :, :2], "gz", True), shift(edges[:, :, 2:], "gz", False)],
            axis=2,
        )
    xm = shift(xu, "gx", True)
    xp = shift(xd, "gx", False)
    parameters = (
        kernel_one, kernel_two, kernel_three,
        bias_one[None], bias_two[None], bias_three[None],
    )
    own, ya, yb, eu, ed = call(
        faces_kernel,
        [
            ((nx, ny * rows, line), BF16), yface, yface,
            ((h, ny, 4, line), BF16), ((h, ny, 4, line), BF16),
        ],
        [pltpu.VMEM((nx, ny, 8, line), F32)],
        flops=8 * 10**9,
        nbytes=10**6,
    )(pairs, edges)
    em = shift(eu, "gx", True)
    ep = shift(ed, "gx", False)
    ya = swap(ya, "gy", True)
    yb = swap(yb, "gy", False)
    tail = jnp.where(is_even("gx"), nx - h, 0)

    def planes(side, start):
        return lax.dynamic_slice_in_dim(side, start, h, axis=0)

    caa = swap(planes(ya, tail), "gx", True)
    cab = swap(planes(ya, nx - h - tail), "gx", False)
    cba = swap(planes(yb, tail), "gx", True)
    cbb = swap(planes(yb, nx - h - tail), "gx", False)
    w1, w2, w3, bias, pattern = call(
        weights_kernel,
        [((18 * c, 4 * c), BF16)] * 3
        + [((3, line), F32), ((4 * nz, 4 * nz), BF16)],
        [pltpu.VMEM((3, 1, c), F32), pltpu.SemaphoreType.DMA((3,))],
        far=3,
        flops=2 * 10**9,
        nbytes=10**6,
    )(*parameters)
    (l1own,) = call(
        lambda o, w, b, l: middle_own(o, w, b, rows, l),
        [((nx - 2, (ny - 2) * rows, line), BF16)],
        flops=10**9,
        nbytes=10**6,
    )(own, w1, bias)
    l1, near = call(
        middle_first,
        [
            ((nx + 4, (ny - 2) * rows, line), BF16),
            ((nx + 6, 4 * rows, line), BF16),
        ],
        [
            pltpu.VMEM((nx + 6, ny * rows, line), BF16),
            pltpu.VMEM((h, ny, 8, line), F32),
        ],
        flops=2 * 10**9,
        nbytes=10**6,
    )(own, xm, xp, em, ep, l1own, w1, bias)
    l2, l3 = call(
        lambda a, v, w, b, o, p: middle_second(a, v, w, b, rows, o, p),
        [
            ((nx + 2, (ny - 4) * rows, line), BF16),
            ((nx, ny - 6, half, line), BF16),
        ],
        flops=2 * 10**9,
        nbytes=10**6,
    )(l1, w2, w3, bias)
    deep = around(3 * rows, 16) + 2 * rows
    strips = [pltpu.VMEM((nx + k, deep, line), BF16) for k in (6, 4, 2)]
    (strip,) = call(
        first_kernel, [((nx, 3, half, line), BF16)], strips,
        flops=4 * 10**9, nbytes=10**6,
    )(near, ya, caa, cab, l1, l2, w1, w2, w3, bias)
    (out,) = call(
        second_kernel,
        [((c, nx, ny, nz), BF16)],
        strips + [pltpu.VMEM((nx, c * ny, nz), F32)],
        flops=4 * 10**9, nbytes=10**6,
    )(near, yb, cba, cbb, l1, l2, strip, l3, w1, w2, w3, bias, pattern)
    return out[None]


def solution(mesh):
    return jax.shard_map(
        shards,
        mesh=mesh,
        in_specs=(P(None, None, "gx", "gy", "gz"), P(), P(), P(), P(), P(), P()),
        out_specs=P(None, None, "gx", "gy", "gz"),
        check_vma=False,
    )
```

```python
import jax
import jax.numpy as jnp
from jax import lax
from jax.experimental import pallas as pl
from jax.experimental.pallas import tpu as pltpu
from jax.sharding import PartitionSpec as P


HALO = 3
SQRT_HALF = 0.7071067811865476
BF16 = jnp.bfloat16
F32 = jnp.float32
VMEM = pl.BlockSpec(memory_space=pltpu.VMEM)


def around(size, step):
    return -(-size // step) * step


def call(kernel, outs, scratch=(), flops=0, nbytes=0, far=0):
    outs = [jax.ShapeDtypeStruct(s, d) for s, d in outs]

    def run(*args):
        args = list(args)
        for i in range(len(args) - far, len(args)):
            args[i] = pltpu.with_memory_space_constraint(args[i], pltpu.HBM)
        return pl.pallas_call(
            kernel,
            out_shape=outs,
            in_specs=[VMEM] * (len(args) - far)
            + [pl.BlockSpec(memory_space=pltpu.HBM)] * far,
            out_specs=[VMEM] * len(outs),
            scratch_shapes=list(scratch),
            cost_estimate=pl.CostEstimate(
                flops=flops, bytes_accessed=nbytes, transcendentals=0
            ),
            compiler_params=pltpu.CompilerParams(vmem_limit_bytes=24 * 1024 * 1024),
        )(*args)

    return run


def gelu(u):
    return 0.5 * u * (1.0 + lax.erf(u * SQRT_HALF))


def iota(shape, dim):
    return lax.broadcasted_iota(jnp.int32, shape, dim)


def is_even(axis):
    return lax.rem(lax.axis_index(axis), 2) == 0


def rows_kernel(field, pairs, edges, xu, xd, planes):
    c, nx, ny, nz = field.shape
    rows = pairs.shape[2]
    h = HALO
    tall = rows + 8
    m = iota((2 * tall, nz), 0)
    second = (m >= tall).astype(jnp.int32)
    m = m - tall * second
    half = nz // 2
    first = jnp.where(m < rows + 2, m - rows + half, m - rows - 1)
    m = jnp.where(m < rows, m, jnp.where(m < rows + 4, first, -8))
    pick = (iota((2 * tall, nz), 1) == 2 * m - 3 + second).astype(F32).astype(BF16)
    for x in range(nx):
        planes[x] = field[:, x].astype(F32).reshape(c * ny, nz)
        for y in range(0, ny, 4):
            lines = [
                planes[x, pl.ds(y + k, c, stride=ny), :].astype(BF16) for k in range(4)
            ]
            r = lax.dot_general(
                pick,
                jnp.concatenate(lines, axis=0),
                (((1,), (1,)), ((), ())),
                preferred_element_type=F32,
            ).astype(BF16)
            for k in range(4):
                lanes = slice(c * k, c * (k + 1))
                line = jnp.concatenate([r[:tall, lanes], r[tall:, lanes]], axis=1)
                pairs[x, y + k] = line[:rows]
                edges[x, y + k] = line[rows : rows + 4]
                if x >= nx - h:
                    xu[x - nx + h, y + k] = line[:rows]
                if x < h:
                    xd[x, y + k] = line[:rows]


def end_rows(lines, edges, wide):
    rows = lines.shape[2]
    wide[:, :, :4] = edges[...].astype(F32)
    got = wide[...]
    row = iota(got.shape, 2)
    low = jnp.where(row < 2, got, 0.0)
    moved = pltpu.roll(got, got.shape[2] - 1, 2)
    high = jnp.where((row >= 1) & (row < 3), moved, 0.0)
    first = lines[:, :, :8].astype(F32) + low
    last = lines[:, :, rows - 8 :].astype(F32) + high
    return first, last


def faces_kernel(pairs, edges, own, ya, yb, eu, ed, wide):
    nx, ny, rows, line = pairs.shape
    h = HALO
    first, last = end_rows(pairs, edges, wide)
    e = jnp.concatenate(
        [first, pairs[:, :, 8 : rows - 8].astype(F32), last], axis=2
    )
    own[...] = e.reshape(nx, ny * rows, line).astype(BF16)
    e = e.astype(BF16)
    ya[...] = e[:, ny - h :]
    yb[...] = e[:, :h]
    eu[...] = edges[nx - h :]
    ed[...] = edges[:h]


def weights_kernel(
    k1, k2, k3, b1, b2, b3, w1, w2, w3, bias, pattern, thin, sems
):
    _, _, taps, o, c = k1.shape
    copies = [
        pltpu.make_async_copy(b, thin.at[i], sems.at[i])
        for i, b in enumerate((b1, b2, b3))
    ]
    for copy in copies:
        copy.start()
    nz = pattern.shape[1] // 4
    pattern[...] = spread_pattern(nz // 2, nz)
    j = iota((taps * o, 8 * o), 0)
    n = iota((taps * o, 8 * o), 1)
    p = n // (4 * o)
    t = n // (2 * o) % 2
    q = n // o % 2
    pick = (j == (p - q + 2 * t) * o + n % o).astype(F32).astype(BF16)
    for k, w in ((k1, w1), (k2, w2), (k3, w3)):
        for a in range(3):
            for e in range(3):
                r = lax.dot_general(
                    k[a, e].reshape(taps * o, c),
                    pick,
                    (((0,), (0,)), ((), ())),
                    preferred_element_type=F32,
                ).astype(BF16)
                at = (a * 3 + e) * 2 * c
                w[at : at + c] = r[:, : 4 * o]
                w[at + c : at + 2 * c] = r[:, 4 * o :]
    for copy in copies:
        copy.wait()
    for i in range(3):
        bias[i : i + 1] = jnp.concatenate([thin[i], thin[i]], axis=1)


def conv(source, x, rows, lines, weight, bias):
    height = around(lines * rows, 16)
    taps = [
        source[x + a, e * rows : e * rows + height] for a in range(3) for e in range(3)
    ]
    both = jnp.dot(jnp.concatenate(taps, axis=1), weight, preferred_element_type=F32)
    u = both[:, :128] + pltpu.roll(both[:, 128:], height - 1, 0) + bias
    return gelu(u).astype(BF16)[: lines * rows]


def middle_own(own, w1, bias, rows, l1):
    lines = own.shape[1] // rows - 2
    for x in range(l1.shape[0]):
        l1[x] = conv(own, x, rows, lines, w1[...], bias[0:1])


def middle_first(own, xm, xp, em, ep, l1own, w1, bias, l1, near, s0, wide):
    h, ny, rows, line = xm.shape
    nx = own.shape[0]
    for at, face, edges in ((0, xm, em), (h + nx, xp, ep)):
        s0[at : at + h] = face[...].reshape(h, ny * rows, line)
        first, last = end_rows(face, edges, wide)
        for i in range(h):
            for y in range(ny):
                s0[at + i, y * rows : y * rows + 8] = first[i, y].astype(BF16)
                s0[at + i, y * rows + rows - 8 : (y + 1) * rows] = last[i, y].astype(
                    BF16
                )
    s0[h : h + nx] = own[...]
    near[:, : 2 * rows] = s0[:, : 2 * rows]
    near[:, 2 * rows :] = s0[:, (ny - 2) * rows :]
    for x in range(nx + 4):
        if 3 <= x < nx + 1:
            l1[x] = l1own[x - 3]
        else:
            l1[x] = conv(s0, x, rows, ny - 2, w1[...], bias[0:1])


def middle_second(l1, w2, w3, bias, rows, l2, l3):
    lines = l1.shape[1] // rows - 2
    half = l3.shape[2]
    for x in range(l2.shape[0]):
        l2[x] = conv(l1, x, rows, lines, w2[...], bias[1:2])
    for x in range(l3.shape[0]):
        y = conv(l2, x, rows, lines - 2, w3[...], bias[2:3])
        for i in range(lines - 2):
            l3[x, i] = y[i * rows : i * rows + half]


def spread_pattern(half, nz):
    r = iota((8 * half, 4 * nz), 0)
    n = iota((8 * half, 4 * nz), 1)
    line = r // half % 4
    hit = (line == n // nz) & (n % nz == 2 * (r % half) + r // (4 * half))
    return hit.astype(F32).astype(BF16)


def edge_strip(below, near, side, ca, cb, l1, l2, ws, bias, s0, s1, s2):
    nx, h, rows, line = side.shape
    close = slice(3 * rows, 5 * rows) if below else slice(0, 2 * rows)
    far = slice(0, 3 * rows) if below else slice(2 * rows, 5 * rows)
    part = slice(0, 2 * rows) if below else slice(2 * rows, 4 * rows)
    end1 = part if below else slice(l1.shape[1] - 2 * rows, l1.shape[1])
    end2 = part if below else slice(l2.shape[1] - 2 * rows, l2.shape[1])
    first = jnp.where(is_even("gx"), h + nx, 0)
    s0[:, close] = near[:, part]
    s0[pl.ds(first, h), far] = ca[...].reshape(h, h * rows, line)
    s0[pl.ds(h + nx - first, h), far] = cb[...].reshape(h, h * rows, line)
    s0[h : h + nx, far] = side[...].reshape(nx, h * rows, line)
    s1[:, close] = l1[:, end1]
    s2[:, close] = l2[:, end2]
    for source, target, i in ((s0, s1, 0), (s1, s2, 1)):
        for x in range(source.shape[0] - 2):
            target[x, far] = conv(source, x, rows, 3, ws[i][...], bias[i : i + 1])
    return [conv(s2, x, rows, 3, ws[2][...], bias[2:3]) for x in range(nx)]


def first_kernel(near, side, ca, cb, l1, l2, w1, w2, w3, bias, out, s0, s1, s2):
    rows = side.shape[2]
    half = out.shape[2]

    def body(below):
        ws = (w1, w2, w3)
        y = edge_strip(below, near, side, ca, cb, l1, l2, ws, bias, s0, s1, s2)
        for x, lines in enumerate(y):
            for i in range(3):
                out[x, i] = lines[i * rows : i * rows + half]

    body(True)


def second_kernel(
    near, side, ca, cb, l1, l2, other, mid, w1, w2, w3, bias, pattern, out,
    s0, s1, s2, stage,
):
    c, nx, ny, nz = out.shape
    rows = side.shape[2]
    half = nz // 2

    def body(below):
        ws = (w1, w2, w3)
        y = edge_strip(below, near, side, ca, cb, l1, l2, ws, bias, s0, s1, s2)
        for x in range(nx):
            mine = [y[x][i * rows : i * rows + half] for i in range(3)]
            theirs = [other[x, i] for i in range(3)]
            inner = [mid[x, i] for i in range(ny - 6)]
            lines = mine + inner + theirs if below else theirs + inner + mine
            parts = [
                jnp.concatenate(lines[first : first + 4], axis=0)
                for first in range(0, ny, 4)
            ]
            sides = [
                jnp.concatenate([p[:, q * c : (q + 1) * c] for p in parts], axis=1)
                for q in range(2)
            ]
            r = lax.dot_general(
                jnp.concatenate(sides, axis=0),
                pattern[...],
                (((0,), (0,)), ((), ())),
                preferred_element_type=F32,
            )
            for i in range(ny):
                stage[x, pl.ds(i, c, stride=ny), :] = r[
                    i // 4 * c : (i // 4 + 1) * c, i % 4 * nz : (i % 4 + 1) * nz
                ]
            out[:, x] = stage[x].reshape(c, ny, nz).astype(BF16)

    body(False)


def shift(x, axis, up):
    count = lax.axis_size(axis)
    pairs = [(i, (i + 1) % count) if up else ((i + 1) % count, i) for i in range(count)]
    return lax.ppermute(x, axis, pairs)


def swap(x, axis, first):
    count = lax.axis_size(axis)
    assert count % 2 == 0
    up = 1 if first else -1
    pairs = [(i, (i + (up if i % 2 == 0 else -up)) % count) for i in range(count)]
    return lax.ppermute(x, axis, pairs)


def shards(field, kernel_one, bias_one, kernel_two, bias_two, kernel_three, bias_three):
    h = HALO
    field = field[0]
    c, nx, ny, nz = field.shape
    rows = around((nz + 2 * h) // 2, 8)
    half = nz // 2
    line = 2 * c

    xface = ((h, ny, rows, line), BF16)
    yface = ((nx, h, rows, line), BF16)
    pairs, edges, xu, xd = call(
        rows_kernel,
        [((nx, ny, rows, line), BF16), ((nx, ny, 4, line), BF16), xface, xface],
        [pltpu.VMEM((nx, c * ny, nz), F32)],
        flops=8 * 10**9,
        nbytes=10**6,
    )(field)
    if lax.axis_size("gz") == 2:
        edges = shift(edges, "gz", True)
    else:
        edges = jnp.concatenate(
            [shift(edges[:, :, :2], "gz", True), shift(edges[:, :, 2:], "gz", False)],
            axis=2,
        )
    xm = shift(xu, "gx", True)
    xp = shift(xd, "gx", False)
    parameters = (
        kernel_one, kernel_two, kernel_three,
        bias_one[None], bias_two[None], bias_three[None],
    )
    own, ya, yb, eu, ed = call(
        faces_kernel,
        [
            ((nx, ny * rows, line), BF16), yface, yface,
            ((h, ny, 4, line), BF16), ((h, ny, 4, line), BF16),
        ],
        [pltpu.VMEM((nx, ny, 8, line), F32)],
        flops=8 * 10**9,
        nbytes=10**6,
    )(pairs, edges)
    em = shift(eu, "gx", True)
    ep = shift(ed, "gx", False)
    ya = shift(ya, "gy", True)
    yb = shift(yb, "gy", False)
    tail = jnp.where(is_even("gx"), nx - h, 0)

    def planes(side, start):
        return lax.dynamic_slice_in_dim(side, start, h, axis=0)

    caa = swap(planes(ya, tail), "gx", True)
    cab = swap(planes(ya, nx - h - tail), "gx", False)
    cba = swap(planes(yb, tail), "gx", True)
    cbb = swap(planes(yb, nx - h - tail), "gx", False)
    w1, w2, w3, bias, pattern = call(
        weights_kernel,
        [((18 * c, 4 * c), BF16)] * 3
        + [((3, line), F32), ((4 * nz, 4 * nz), BF16)],
        [pltpu.VMEM((3, 1, c), F32), pltpu.SemaphoreType.DMA((3,))],
        far=3,
        flops=2 * 10**9,
        nbytes=10**6,
    )(*parameters)
    (l1own,) = call(
        lambda o, w, b, l: middle_own(o, w, b, rows, l),
        [((nx - 2, (ny - 2) * rows, line), BF16)],
        flops=10**9,
        nbytes=10**6,
    )(own, w1, bias)
    l1, near = call(
        middle_first,
        [
            ((nx + 4, (ny - 2) * rows, line), BF16),
            ((nx + 6, 4 * rows, line), BF16),
        ],
        [
            pltpu.VMEM((nx + 6, ny * rows, line), BF16),
            pltpu.VMEM((h, ny, 8, line), F32),
        ],
        flops=2 * 10**9,
        nbytes=10**6,
    )(own, xm, xp, em, ep, l1own, w1, bias)
    l2, l3 = call(
        lambda a, v, w, b, o, p: middle_second(a, v, w, b, rows, o, p),
        [
            ((nx + 2, (ny - 4) * rows, line), BF16),
            ((nx, ny - 6, half, line), BF16),
        ],
        flops=2 * 10**9,
        nbytes=10**6,
    )(l1, w2, w3, bias)
    deep = around(3 * rows, 16) + 2 * rows
    strips = [pltpu.VMEM((nx + k, deep, line), BF16) for k in (6, 4, 2)]
    (strip,) = call(
        first_kernel, [((nx, 3, half, line), BF16)], strips,
        flops=4 * 10**9, nbytes=10**6,
    )(near, ya, caa, cab, l1, l2, w1, w2, w3, bias)
    (out,) = call(
        second_kernel,
        [((c, nx, ny, nz), BF16)],
        strips + [pltpu.VMEM((nx, c * ny, nz), F32)],
        flops=4 * 10**9, nbytes=10**6,
    )(near, yb, cba, cbb, l1, l2, strip, l3, w1, w2, w3, bias, pattern)
    return out[None]


def solution(mesh):
    return jax.shard_map(
        shards,
        mesh=mesh,
        in_specs=(P(None, None, "gx", "gy", "gz"), P(), P(), P(), P(), P(), P()),
        out_specs=P(None, None, "gx", "gy", "gz"),
        check_vma=False,
    )
```
